32 devices in a mesh: grp: 4 (over y, x), seq: 8 (over z, core).
Axes of the slice: x: 2, y: 2, z: 4, core: 2. Of those that a mesh axis runs over, the one named last changes fastest.
Arguments:
- queries: bfloat16 [8192, 2048], P(('grp', 'seq')), may hold values from -48 to 48
- key_rows: bfloat16 [8192, 512], P(('grp', 'seq')), may hold values from -4.5 to 4.5
- value_rows: bfloat16 [8192, 512], P(('grp', 'seq')), may hold values from -6 to 6
- segments: int32 [8192], P(('grp', 'seq')), may hold values from 0 to 3, as said below
Outputs:
- attended: bfloat16 [8192, 2048], P(('grp', 'seq'))
- log_sums: float32 [16, 8192], P(None, ('grp', 'seq'))
The draws below stay inside these ranges and needn't reach their ends.
Inputs may be any that keep to these rules, and one draw needn't show every extreme that they name: `segments`: never falls along the sequence, starts at 0 and rises by one at each new document; the last token holds the largest value.
All inputs are finite; a program needn't handle non-finite values.
Results may differ from the reference program's by a relative error of at most 0.0035.
Values may be sent and summed in bfloat16 or wider, within the bound.
A program may use at most 192 MiB of HBM per device.

```python
import math
import jax
import jax.numpy as jnp
from jax import lax

Q_HEADS = 16
KV_HEADS = 4
HEAD_DIM = 128
WINDOW = 4096
TOK_DEV = 256
SEQ_LEN = 8192


def boundary_flags(key):
    stretch = max(WINDOW // 2, 2)
    pieces = SEQ_LEN // stretch
    offsets = jax.random.randint(jax.random.fold_in(key, 11), (pieces,), 1, stretch)
    spots = jnp.arange(SEQ_LEN)
    first_mark = SEQ_LEN // 2 - TOK_DEV // 2
    second_mark = SEQ_LEN // 2 + TOK_DEV // 2
    low_piece = first_mark // stretch
    high_piece = min(pieces - 1, (second_mark + WINDOW) // stretch)
    piece_of = spots // stretch
    kept = (piece_of < low_piece) | (piece_of > high_piece)
    flags = (kept & (spots % stretch == offsets[piece_of])).astype(jnp.int32)
    flags = jnp.where((spots == first_mark) | (spots == second_mark), 1, flags)
    return flags.at[0].set(0)


def draw_segments(key, part):
    return jnp.cumsum(boundary_flags(key)).astype(jnp.int32)


def query_key_pair(key):
    group = Q_HEADS // KV_HEADS
    keys = jnp.clip(jax.random.normal(jax.random.fold_in(key, 21), (SEQ_LEN, KV_HEADS, HEAD_DIM), jnp.float32), -4.5, 4.5)
    queries = jnp.clip(3.0 * jax.random.normal(jax.random.fold_in(key, 22), (SEQ_LEN, KV_HEADS, group, HEAD_DIM), jnp.float32), -18.0, 18.0)
    return (queries.reshape(SEQ_LEN, Q_HEADS * HEAD_DIM).astype(jnp.bfloat16), keys.reshape(SEQ_LEN, KV_HEADS * HEAD_DIM).astype(jnp.bfloat16))


def draw_queries(key, part):
    return query_key_pair(key)[0]


def draw_key_rows(key, part):
    return query_key_pair(key)[1]


def steps_of(rng, extent, split, least, top_value):
    gain, own = 1.0, jax.random.fold_in(rng, 6)
    for position, blocks in split:
        heights = jnp.exp(jax.random.uniform(jax.random.fold_in(own, position), (blocks,), jnp.float32, least / len(split), top_value / len(split)))
        gain = gain * jnp.repeat(heights, extent[position] // blocks).reshape([-1 if axis == position else 1 for axis in range(len(extent))])
    return gain


def centred(key, dims, deviation, bound, cuts=(), kind=jnp.bfloat16):
    entries = jax.random.normal(key, dims, jnp.float32) * deviation
    if len(cuts) > 0:
        entries = steps_of(key, dims, cuts, -0.22, 0.18) * entries
    return jnp.clip(entries, min=-bound, max=bound).astype(kind)


def setup_inputs(seed: int = 0) -> dict:
    splits = jax.random.split(jax.random.key(seed), 5)
    return {
        "queries": draw_queries(jax.random.fold_in(splits[4], 71), 0),
        "key_rows": draw_key_rows(jax.random.fold_in(splits[4], 71), 0),
        "value_rows": centred(splits[2], (SEQ_LEN, KV_HEADS * HEAD_DIM), 1.0, 6.0, ((0, 32),)),
        "segments": draw_segments(jax.random.fold_in(splits[4], 71), 0),
    }


def reference(queries, key_rows, value_rows, segments):
    group = Q_HEADS // KV_HEADS
    block = math.gcd(SEQ_LEN, 512)
    count = SEQ_LEN // block
    span = block + WINDOW
    scale = 1.0 / math.sqrt(HEAD_DIM)
    width = KV_HEADS * HEAD_DIM
    key_pad = jnp.concatenate([jnp.zeros((WINDOW, width), key_rows.dtype), key_rows], axis=0)
    value_pad = jnp.concatenate([jnp.zeros((WINDOW, width), value_rows.dtype), value_rows], axis=0)
    seg_pad = jnp.concatenate([jnp.full((WINDOW,), -1, jnp.int32), segments.astype(jnp.int32)], axis=0)

    def one_block(index):
        first = (index * block).astype(jnp.int32)
        q_part = lax.dynamic_slice_in_dim(queries, first, block, 0).reshape(block, KV_HEADS, group, HEAD_DIM).astype(jnp.float32)
        k_part = lax.dynamic_slice_in_dim(key_pad, first, span, 0).reshape(span, KV_HEADS, HEAD_DIM).astype(jnp.float32)
        v_part = lax.dynamic_slice_in_dim(value_pad, first, span, 0).reshape(span, KV_HEADS, HEAD_DIM).astype(jnp.float32)
        q_seg = lax.dynamic_slice_in_dim(segments.astype(jnp.int32), first, block, 0)
        k_seg = lax.dynamic_slice_in_dim(seg_pad, first, span, 0)
        q_pos = first + jnp.arange(block, dtype=jnp.int32)
        k_pos = first - WINDOW + jnp.arange(span, dtype=jnp.int32)
        allowed = (k_pos[None, :] <= q_pos[:, None]) & (k_pos[None, :] > q_pos[:, None] - WINDOW) & (k_seg[None, :] == q_seg[:, None])
        scores = jnp.einsum('tkgd,lkd->kgtl', q_part, k_part, precision=lax.Precision.HIGHEST) * scale
        masked = jnp.where(allowed, scores, -1e+30)
        top = lax.optimization_barrier(jnp.max(masked, axis=-1))
        expo = jnp.where(allowed, jnp.exp(masked - top[..., None]), 0.0)
        total = lax.optimization_barrier(jnp.sum(expo, axis=-1))
        weights = lax.optimization_barrier(expo.astype(jnp.bfloat16))
        summed = jnp.einsum('kgtl,lkd->tkgd', weights.astype(jnp.float32), v_part, precision=lax.Precision.HIGHEST)
        out = summed / jnp.transpose(total, (2, 0, 1))[..., None]
        out = out.reshape(block, Q_HEADS * HEAD_DIM).astype(jnp.bfloat16)
        sums = (top + jnp.log(total)).reshape(Q_HEADS, block)
        return (out, sums)
    outs, sums = lax.map(one_block, jnp.arange(count, dtype=jnp.int32))
    attended = outs.reshape(SEQ_LEN, Q_HEADS * HEAD_DIM)
    log_sums = jnp.transpose(sums, (1, 0, 2)).reshape(Q_HEADS, SEQ_LEN)
    return (attended, log_sums)
```

```python
import math

import jax
import jax.numpy as jnp
from jax import lax
from jax.experimental import pallas as pl
from jax.experimental.pallas import tpu as pltpu
from jax.sharding import PartitionSpec as P

Q_HEADS = 16
KV_HEADS = 4
HEAD_DIM = 128
WINDOW = 4096
AXES = ("grp", "seq")
LOW = -1e30


def head_step(h, qt, k_ref, vt, m_ref, l_ref, acc, bias):
    c = math.log2(math.e) / math.sqrt(HEAD_DIM)
    g = h // (Q_HEADS // KV_HEADS)
    s = jnp.dot(k_ref[:, g * HEAD_DIM : (g + 1) * HEAD_DIM], qt[h], preferred_element_type=jnp.float32)
    if bias is not None:
        s = s + bias[...]
    m_old = m_ref[h]
    m_new = jnp.maximum(m_old, jnp.max(s, axis=0, keepdims=True))
    p = jnp.exp2((s - m_new) * c)
    alpha = jnp.exp2((m_old - m_new) * c)
    l_ref[h] = l_ref[h] * alpha + jnp.sum(p, axis=0, keepdims=True)
    m_ref[h] = m_new
    acc[h] = acc[h] * alpha + jnp.dot(vt, p.astype(jnp.bfloat16), preferred_element_type=jnp.float32)


def block_step(qt, k_ref, v_ref, m_ref, l_ref, acc, bias):
    group = Q_HEADS // KV_HEADS
    for g in range(KV_HEADS):
        vt = v_ref[:, g * HEAD_DIM : (g + 1) * HEAD_DIM].T
        for h in range(g * group, (g + 1) * group):
            head_step(h, qt, k_ref, vt, m_ref, l_ref, acc, bias)


def flash(info, lower_ref, q_ref, k_ref, v_ref, o_ref, ls_ref, qt, m_ref, l_ref, acc, bias):
    j = pl.program_id(0)
    tok = q_ref.shape[0]
    device, first, clean = info[0], info[1], info[2]

    @pl.when(j == 0)
    def _():
        for h in range(Q_HEADS):
            qt[h] = q_ref[:, h * HEAD_DIM : (h + 1) * HEAD_DIM].T
        m_ref[...] = jnp.full_like(m_ref, LOW)
        l_ref[...] = jnp.zeros_like(l_ref)
        acc[...] = jnp.zeros_like(acc)

    block = device - j
    edge = (j == 0) | (block < clean)

    @pl.when((block >= first) & edge)
    def _():
        key_pos = block * tok + lax.broadcasted_iota(jnp.int32, (tok, tok), 0)
        pos = device * tok + lax.broadcasted_iota(jnp.int32, (tok, tok), 1)
        allowed = (key_pos >= lower_ref[...]) & (key_pos <= pos)
        bias[...] = jnp.where(allowed, 0.0, LOW)
        block_step(qt, k_ref, v_ref, m_ref, l_ref, acc, bias)

    @pl.when((block >= first) & jnp.logical_not(edge))
    def _():
        block_step(qt, k_ref, v_ref, m_ref, l_ref, acc, None)

    @pl.when(j == pl.num_programs(0) - 1)
    def _():
        for h in range(Q_HEADS):
            out = acc[h] * (1.0 / l_ref[h])
            o_ref[:, h * HEAD_DIM : (h + 1) * HEAD_DIM] = out.T.astype(o_ref.dtype)
            ls_ref[h : h + 1, :] = m_ref[h] * (1.0 / math.sqrt(HEAD_DIM)) + jnp.log(l_ref[h])


def on_device(queries, key_rows, value_rows, segments):
    tok = queries.shape[0]
    width = key_rows.shape[1]
    device = lax.axis_index(AXES)
    k_all = lax.all_gather(key_rows, AXES, tiled=True)
    v_all = lax.all_gather(value_rows, AXES, tiled=True)
    seg_all = lax.all_gather(segments, AXES, tiled=True)
    starts = jnp.sum((seg_all[:, None] < segments[None, :]).astype(jnp.int32), axis=0)
    positions = device * tok + jnp.arange(tok, dtype=jnp.int32)
    lower = jnp.maximum(starts, positions - WINDOW + 1)
    first = jnp.min(lower) // tok
    clean = (jnp.max(lower) + tok - 1) // tok
    info = jnp.stack([device, first, clean]).astype(jnp.int32)
    reach = (WINDOW - 1 + tok - 1) // tok + 1

    def kv_index(j, info):
        return (jnp.maximum(info[0] - j, info[1]), 0)

    const = lambda j, info: (0, 0)
    return pl.pallas_call(
        flash,
        grid_spec=pltpu.PrefetchScalarGridSpec(
            num_scalar_prefetch=1,
            grid=(reach,),
            in_specs=[
                pl.BlockSpec((1, tok), const),
                pl.BlockSpec(queries.shape, const),
                pl.BlockSpec((tok, width), kv_index),
                pl.BlockSpec((tok, width), kv_index),
            ],
            out_specs=[
                pl.BlockSpec(queries.shape, const),
                pl.BlockSpec((Q_HEADS, tok), const),
            ],
            scratch_shapes=[
                pltpu.VMEM((Q_HEADS, HEAD_DIM, tok), jnp.bfloat16),
                pltpu.VMEM((Q_HEADS, 1, tok), jnp.float32),
                pltpu.VMEM((Q_HEADS, 1, tok), jnp.float32),
                pltpu.VMEM((Q_HEADS, HEAD_DIM, tok), jnp.float32),
                pltpu.VMEM((tok, tok), jnp.float32),
            ],
        ),
        out_shape=[
            jax.ShapeDtypeStruct(queries.shape, jnp.bfloat16),
            jax.ShapeDtypeStruct((Q_HEADS, tok), jnp.float32),
        ],
        compiler_params=pltpu.CompilerParams(dimension_semantics=("arbitrary",)),
    )(info, lower[None, :], queries, k_all, v_all)


def solution(mesh):
    in_specs = (P(AXES, None), P(AXES, None), P(AXES, None), P(AXES))
    out_specs = (P(AXES, None), P(None, AXES))
    return jax.shard_map(
        on_device, mesh=mesh, in_specs=in_specs, out_specs=out_specs, check_vma=False
    )
```

```python
import functools
import math

import jax
import jax.numpy as jnp
from jax import lax
from jax.experimental import pallas as pl
from jax.experimental.pallas import tpu as pltpu
from jax.sharding import PartitionSpec as P

Q_HEADS = 16
KV_HEADS = 4
HEAD_DIM = 128
WINDOW = 4096
AXES = ("grp", "seq")
LOW = -1e30


def head_step(h, qt, k_ref, vt, m_ref, l_ref, acc, bias):
    c = math.log2(math.e) / math.sqrt(HEAD_DIM)
    g = h // (Q_HEADS // KV_HEADS)
    s = jnp.dot(k_ref[:, g * HEAD_DIM : (g + 1) * HEAD_DIM], qt[h], preferred_element_type=jnp.float32)
    if bias is not None:
        s = s + bias[...]
    m_old = m_ref[h]
    m_new = jnp.maximum(m_old, jnp.max(s, axis=0, keepdims=True))
    p = jnp.exp2((s - m_new) * c)
    alpha = jnp.exp2((m_old - m_new) * c)
    l_ref[h] = l_ref[h] * alpha + jnp.sum(p, axis=0, keepdims=True)
    m_ref[h] = m_new
    acc[h] = acc[h] * alpha + jnp.dot(vt, p.astype(jnp.bfloat16), preferred_element_type=jnp.float32)


def block_step(qt, k_ref, v_ref, m_ref, l_ref, acc, bias):
    group = Q_HEADS // KV_HEADS
    for g in range(KV_HEADS):
        vt = v_ref[:, g * HEAD_DIM : (g + 1) * HEAD_DIM].T
        for h in range(g * group, (g + 1) * group):
            head_step(h, qt, k_ref, vt, m_ref, l_ref, acc, bias)


def flash(info, lower_ref, q_ref, k_ref, v_ref, o_ref, ls_ref, qt, m_ref, l_ref, acc, bias):
    j = pl.program_id(0)
    tok = q_ref.shape[0]
    device, first, clean = info[0], info[1], info[2]

    @pl.when(j == 0)
    def _():
        for h in range(Q_HEADS):
            qt[h] = q_ref[:, h * HEAD_DIM : (h + 1) * HEAD_DIM].T
        m_ref[...] = jnp.full_like(m_ref, LOW)
        l_ref[...] = jnp.zeros_like(l_ref)
        acc[...] = jnp.zeros_like(acc)

    block = device - j
    edge = (j == 0) | (block < clean)

    @pl.when((block >= first) & edge)
    def _():
        key_pos = block * tok + lax.broadcasted_iota(jnp.int32, (tok, tok), 0)
        pos = device * tok + lax.broadcasted_iota(jnp.int32, (tok, tok), 1)
        allowed = (key_pos >= lower_ref[...]) & (key_pos <= pos)
        bias[...] = jnp.where(allowed, 0.0, LOW)
        block_step(qt, k_ref, v_ref, m_ref, l_ref, acc, bias)

    @pl.when((block >= first) & jnp.logical_not(edge))
    def _():
        block_step(qt, k_ref, v_ref, m_ref, l_ref, acc, None)

    @pl.when(j == pl.num_programs(0) - 1)
    def _():
        for h in range(Q_HEADS):
            out = acc[h] * (1.0 / l_ref[h])
            o_ref[:, h * HEAD_DIM : (h + 1) * HEAD_DIM] = out.T.astype(o_ref.dtype)
            ls_ref[h : h + 1, :] = m_ref[h] * (1.0 / math.sqrt(HEAD_DIM)) + jnp.log(l_ref[h])


def spread(grp_n, k_in, v_in, s_in, k_out, v_out, s_out, send, recv, own):
    seq_n = k_out.shape[0] // 3
    chips = seq_n // 2
    c, s = lax.axis_index("grp"), lax.axis_index("seq")
    z, core = s // 2, s % 2
    even = c % 2 == 0
    srcs, bufs = (k_in, v_in, s_in), (k_out, v_out, s_out)
    sib = s + 1 - 2 * core
    pair = c + 1 - 2 * (c % 2)
    peers = (
        (z + 1 < chips, (c, s + 2)),
        (z > 0, (c, s - 2)),
        (c >= 0, (pair, s)),
        (c + 2 < grp_n, (c + 2, s)),
        (c >= 2, (c - 2, s)),
        (c >= 0, (c, sib)),
    )
    barrier = pltpu.get_barrier_semaphore()
    count = 0
    for ok, to in peers:
        count = count + ok.astype(jnp.int32)

        @pl.when(ok)
        def _(to=to):
            pl.semaphore_signal(barrier, inc=1, device_id=to, device_id_type=pl.DeviceIdType.MESH)

    pl.semaphore_wait(barrier, count)

    def slot(dc, zz, cc):
        return (2 - dc) * seq_n + 2 * zz + cc

    def copy(t, kind, zz, src_slot, dst_slot, to, source=None):
        src = bufs[t].at[src_slot] if source is None else source
        return pltpu.make_async_remote_copy(
            src_ref=src,
            dst_ref=bufs[t].at[dst_slot],
            send_sem=send.at[kind, zz, t],
            recv_sem=recv.at[dst_slot, t],
            device_id=to,
            device_id_type=pl.DeviceIdType.MESH,
        )

    def sends(dc, zz, t, act, mine=False):
        here = slot(dc, zz, core)
        source = srcs[t] if mine else None

        def go(ok, kind, dst, to):
            @pl.when(ok)
            def _():
                act(copy(t, kind, zz, here, dst, to, source))

        if dc == 0:
            go((zz <= z) & (z + 1 < chips), 0, here, (c, s + 2))
            go((zz >= z) & (z > 0), 1, here, (c, s - 2))
            go((c + 2 < grp_n) & (jnp.logical_not(even) | (zz >= z)), 3, slot(2, zz, core), (c + 2, s))
            go(even, 2, slot(1, zz, core), (c + 1, s))
            go(zz <= z, 4, here, (c, sib))
        elif dc == 1:
            go(zz >= 0, 5, here, (c, sib))
        else:
            go(jnp.logical_not(even), 7, slot(1, zz, core), (c - 1, s))
            go(zz >= z, 6, here, (c, sib))

    def present(dc, zz):
        inside = (zz >= 0) & (zz < chips)
        if dc == 0:
            return inside
        if dc == 1:
            return inside & (c >= 1)
        return inside & (c >= 2) & (jnp.logical_not(even) | (zz >= z))

    def arrived(dc, zz, cc, t):
        here = slot(dc, zz, cc)
        pltpu.make_async_remote_copy(
            src_ref=bufs[t].at[here],
            dst_ref=bufs[t].at[here],
            send_sem=send.at[0, 0, t],
            recv_sem=recv.at[here, t],
            device_id=(c, sib),
            device_id_type=pl.DeviceIdType.MESH,
        ).wait_recv()

    def local(t):
        return pltpu.make_async_copy(srcs[t], bufs[t].at[slot(0, z, core)], own.at[t])

    for t in range(3):
        sends(0, z, t, lambda d: d.start(), True)
    for t in range(3):
        local(t).start()

    def event(dc, zz):
        @pl.when(present(dc, zz))
        def _():
            for t in range(3):
                arrived(dc, zz, core, t)
                sends(dc, zz, t, lambda d: d.start())

    for r in range(1, chips + 1):
        if r < chips:
            event(0, z - r)
            event(0, z + r)
        for sign in (-1, 1) if r > 1 else (1,):
            event(2, z + sign * (r - 1))
            event(1, z + sign * (r - 1))

    for zz in range(chips):
        for dc in range(3):
            zv = zz + 0 * z

            def finish(dc=dc, zv=zv):
                for t in range(3):
                    sends(dc, zv, t, lambda d: d.wait_send())

            if dc == 0:
                finish()
            else:
                pl.when(present(dc, zv))(finish)
            theirs = (zv <= z) if dc == 0 else (c >= 1) if dc == 1 else (c >= 2) & (zv >= z)

            @pl.when(theirs)
            def _(dc=dc, zv=zv):
                for t in range(3):
                    arrived(dc, zv, 1 - core, t)

    for t in range(3):
        local(t).wait()


def gather_rows(key_rows, value_rows, segments):
    grp_n, seq_n = lax.axis_size("grp"), lax.axis_size("seq")
    tok, width = key_rows.shape
    hbm = pl.BlockSpec(memory_space=pl.ANY)
    slots = 3 * seq_n
    return pl.pallas_call(
        functools.partial(spread, grp_n),
        out_shape=[
            jax.ShapeDtypeStruct((slots, tok, width), jnp.bfloat16),
            jax.ShapeDtypeStruct((slots, tok, width), jnp.bfloat16),
            jax.ShapeDtypeStruct((slots, 1, tok), jnp.int32),
        ],
        in_specs=[hbm] * 3,
        out_specs=[hbm] * 3,
        scratch_shapes=[
            pltpu.SemaphoreType.DMA((8, seq_n // 2, 3)),
            pltpu.SemaphoreType.DMA((slots, 3)),
            pltpu.SemaphoreType.DMA((3,)),
        ],
        compiler_params=pltpu.CompilerParams(collective_id=0, has_side_effects=True),
    )(key_rows, value_rows, segments[None, :])


def on_device(queries, key_rows, value_rows, segments):
    tok = queries.shape[0]
    grp_n, seq_n = lax.axis_size("grp"), lax.axis_size("seq")
    device = lax.axis_index(AXES)
    offset = device * tok
    if 2 * seq_n * tok == WINDOW and grp_n % 2 == 0 and seq_n % 2 == 0:
        k_all, v_all, seg_all = gather_rows(key_rows, value_rows, segments)
        base = (lax.axis_index("grp") - 2) * seq_n
    else:
        k_all = lax.all_gather(key_rows, AXES)
        v_all = lax.all_gather(value_rows, AXES)
        seg_all = lax.all_gather(segments, AXES)
        base = 0
    seg_all = seg_all.reshape(-1)
    key_pos = base * tok + jnp.arange(seg_all.shape[0], dtype=jnp.int32)
    begin = jnp.maximum(offset - WINDOW, 0)
    before = (key_pos >= begin) & (key_pos < offset) & (seg_all < segments[0])
    carried = begin + jnp.sum(before.astype(jnp.int32))
    inner = jnp.sum((segments[:, None] < segments[None, :]).astype(jnp.int32), axis=0)
    starts = jnp.where(segments == segments[0], carried, offset + inner)
    positions = offset + jnp.arange(tok, dtype=jnp.int32)
    lower = jnp.maximum(starts, positions - WINDOW + 1)
    first = jnp.min(lower) // tok
    clean = (jnp.max(lower) + tok - 1) // tok
    info = jnp.stack([device, first, clean, device - base]).astype(jnp.int32)
    reach = (WINDOW - 1 + tok - 1) // tok + 1
    return attention(info, lower, queries, k_all, v_all, reach)


def attention(info, lower, queries, k_all, v_all, reach):
    tok = queries.shape[0]
    width = k_all.shape[2]

    def kv_index(j, info):
        return (jnp.maximum(info[3] - j, info[3] - info[0] + info[1]), 0, 0)

    const = lambda j, info: (0, 0)
    return pl.pallas_call(
        flash,
        grid_spec=pltpu.PrefetchScalarGridSpec(
            num_scalar_prefetch=1,
            grid=(reach,),
            in_specs=[
                pl.BlockSpec((1, tok), const),
                pl.BlockSpec(queries.shape, const),
                pl.BlockSpec((None, tok, width), kv_index),
                pl.BlockSpec((None, tok, width), kv_index),
            ],
            out_specs=[
                pl.BlockSpec(queries.shape, const),
                pl.BlockSpec((Q_HEADS, tok), const),
            ],
            scratch_shapes=[
                pltpu.VMEM((Q_HEADS, HEAD_DIM, tok), jnp.bfloat16),
                pltpu.VMEM((Q_HEADS, 1, tok), jnp.float32),
                pltpu.VMEM((Q_HEADS, 1, tok), jnp.float32),
                pltpu.VMEM((Q_HEADS, HEAD_DIM, tok), jnp.float32),
                pltpu.VMEM((tok, tok), jnp.float32),
            ],
        ),
        out_shape=[
            jax.ShapeDtypeStruct(queries.shape, jnp.bfloat16),
            jax.ShapeDtypeStruct((Q_HEADS, tok), jnp.float32),
        ],
        compiler_params=pltpu.CompilerParams(dimension_semantics=("arbitrary",)),
    )(info, lower[None, :], queries, k_all, v_all)


def solution(mesh):
    in_specs = (P(AXES, None), P(AXES, None), P(AXES, None), P(AXES))
    out_specs = (P(AXES, None), P(None, AXES))
    return jax.shard_map(
        on_device, mesh=mesh, in_specs=in_specs, out_specs=out_specs, check_vma=False
    )
```

```python
import functools
import math

import jax
import jax.numpy as jnp
from jax import lax
from jax.experimental import pallas as pl
from jax.experimental.pallas import tpu as pltpu
from jax.sharding import PartitionSpec as P

Q_HEADS = 16
KV_HEADS = 4
HEAD_DIM = 128
WINDOW = 4096
AXES = ("grp", "seq")
LOW = -1e30


def block_step(qt, k_ref, v_ref, m_ref, l_ref, acc, bias):
    c = math.log2(math.e) / math.sqrt(HEAD_DIM)
    group = Q_HEADS // KV_HEADS

    def scores(h):
        g = h // group
        return jnp.dot(
            k_ref[:, g * HEAD_DIM : (g + 1) * HEAD_DIM], qt[h], preferred_element_type=jnp.float32
        )

    def summed(h, p, alpha):
        g = h // group
        if h % group == 0:
            vts[g] = v_ref[:, g * HEAD_DIM : (g + 1) * HEAD_DIM].T
        acc[h] = acc[h] * alpha + jnp.dot(vts[g], p, preferred_element_type=jnp.float32)

    vts = {}
    AHEAD = 2
    ready = [scores(h) for h in range(AHEAD)]
    waiting = None
    for h in range(Q_HEADS):
        if h + AHEAD < Q_HEADS:
            ready.append(scores(h + AHEAD))
        s = ready.pop(0)
        if bias is not None:
            s = s + bias[...]
        m_old = m_ref[h]
        m_new = jnp.maximum(m_old, jnp.max(s, axis=0, keepdims=True))
        p = jnp.exp2((s - m_new) * c)
        alpha = jnp.exp2((m_old - m_new) * c)
        l_ref[h] = l_ref[h] * alpha + jnp.sum(p, axis=0, keepdims=True)
        m_ref[h] = m_new
        if waiting is not None:
            summed(*waiting)
        waiting = (h, p.astype(jnp.bfloat16), alpha)
    summed(*waiting)


def flash(info, lower_ref, q_ref, k_ref, v_ref, o_ref, ls_ref, qt, m_ref, l_ref, acc, bias):
    j = pl.program_id(0)
    tok = q_ref.shape[0]
    device, first, clean = info[0], info[1], info[2]

    @pl.when(j == 0)
    def _():
        for h in range(Q_HEADS):
            qt[h] = q_ref[:, h * HEAD_DIM : (h + 1) * HEAD_DIM].T
        m_ref[...] = jnp.full_like(m_ref, LOW)
        l_ref[...] = jnp.zeros_like(l_ref)
        acc[...] = jnp.zeros_like(acc)

    block = device - j
    edge = (j == 0) | (block < clean)

    @pl.when((block >= first) & edge)
    def _():
        key_pos = block * tok + lax.broadcasted_iota(jnp.int32, (tok, tok), 0)
        pos = device * tok + lax.broadcasted_iota(jnp.int32, (tok, tok), 1)
        allowed = (key_pos >= lower_ref[...]) & (key_pos <= pos)
        bias[...] = jnp.where(allowed, 0.0, LOW)
        block_step(qt, k_ref, v_ref, m_ref, l_ref, acc, bias)

    @pl.when((block >= first) & jnp.logical_not(edge))
    def _():
        block_step(qt, k_ref, v_ref, m_ref, l_ref, acc, None)

    @pl.when(j == pl.num_programs(0) - 1)
    def _():
        for h in range(Q_HEADS):
            out = acc[h] * (1.0 / l_ref[h])
            o_ref[:, h * HEAD_DIM : (h + 1) * HEAD_DIM] = out.T.astype(o_ref.dtype)
            ls_ref[h : h + 1, :] = m_ref[h] * (1.0 / math.sqrt(HEAD_DIM)) + jnp.log(l_ref[h])


def spread(grp_n, k_in, v_in, s_in, k_out, v_out, s_out, send, recv, own):
    seq_n = k_out.shape[0] // 3
    chips = seq_n // 2
    c, s = lax.axis_index("grp"), lax.axis_index("seq")
    z, core = s // 2, s % 2
    even = c % 2 == 0
    srcs, bufs = (k_in, v_in, s_in), (k_out, v_out, s_out)
    sib = s + 1 - 2 * core
    pair = c + 1 - 2 * (c % 2)
    peers = (
        (z + 1 < chips, (c, s + 2)),
        (z > 0, (c, s - 2)),
        (c >= 0, (pair, s)),
        (c + 2 < grp_n, (c + 2, s)),
        (c >= 2, (c - 2, s)),
        (c >= 0, (c, sib)),
    )
    barrier = pltpu.get_barrier_semaphore()
    count = 0
    for ok, to in peers:
        count = count + ok.astype(jnp.int32)

        @pl.when(ok)
        def _(to=to):
            pl.semaphore_signal(barrier, inc=1, device_id=to, device_id_type=pl.DeviceIdType.MESH)

    pl.semaphore_wait(barrier, count)

    def slot(dc, zz, cc):
        return (2 - dc) * seq_n + 2 * zz + cc

    def copy(t, kind, zz, src_slot, dst_slot, to, source=None):
        src = bufs[t].at[src_slot] if source is None else source
        return pltpu.make_async_remote_copy(
            src_ref=src,
            dst_ref=bufs[t].at[dst_slot],
            send_sem=send.at[kind, zz, t],
            recv_sem=recv.at[dst_slot, t],
            device_id=to,
            device_id_type=pl.DeviceIdType.MESH,
        )

    def sends(dc, zz, t, act, mine=False):
        here = slot(dc, zz, core)
        source = srcs[t] if mine else None

        def go(ok, kind, dst, to):
            @pl.when(ok)
            def _():
                act(copy(t, kind, zz, here, dst, to, source))

        if dc == 0:
            go((zz <= z) & (z + 1 < chips), 0, here, (c, s + 2))
            go((zz >= z) & (z > 0), 1, here, (c, s - 2))
            go((c + 2 < grp_n) & (jnp.logical_not(even) | (zz >= z)), 3, slot(2, zz, core), (c + 2, s))
            go(even, 2, slot(1, zz, core), (c + 1, s))
            go(zz <= z, 4, here, (c, sib))
        elif dc == 1:
            go(zz >= 0, 5, here, (c, sib))
        else:
            go(jnp.logical_not(even), 7, slot(1, zz, core), (c - 1, s))
            go(zz >= z, 6, here, (c, sib))

    def present(dc, zz):
        inside = (zz >= 0) & (zz < chips)
        if dc == 0:
            return inside
        if dc == 1:
            return inside & (c >= 1)
        return inside & (c >= 2) & (jnp.logical_not(even) | (zz >= z))

    def arrived(dc, zz, cc, t):
        here = slot(dc, zz, cc)
        pltpu.make_async_remote_copy(
            src_ref=bufs[t].at[here],
            dst_ref=bufs[t].at[here],
            send_sem=send.at[0, 0, t],
            recv_sem=recv.at[here, t],
            device_id=(c, sib),
            device_id_type=pl.DeviceIdType.MESH,
        ).wait_recv()

    def local(t):
        return pltpu.make_async_copy(srcs[t], bufs[t].at[slot(0, z, core)], own.at[t])

    for t in range(3):
        sends(0, z, t, lambda d: d.start(), True)
    for t in range(3):
        local(t).start()

    def event(dc, zz):
        @pl.when(present(dc, zz))
        def _():
            for t in range(3):
                arrived(dc, zz, core, t)
                sends(dc, zz, t, lambda d: d.start())

    for r in range(1, chips + 1):
        if r < chips:
            event(0, z - r)
            event(0, z + r)
        for sign in (-1, 1) if r > 1 else (1,):
            event(2, z + sign * (r - 1))
            event(1, z + sign * (r - 1))

    for zz in range(chips):
        for dc in range(3):
            zv = zz + 0 * z

            def finish(dc=dc, zv=zv):
                for t in range(3):
                    sends(dc, zv, t, lambda d: d.wait_send())

            if dc == 0:
                finish()
            else:
                pl.when(present(dc, zv))(finish)
            theirs = (zv <= z) if dc == 0 else (c >= 1) if dc == 1 else (c >= 2) & (zv >= z)

            @pl.when(theirs)
            def _(dc=dc, zv=zv):
                for t in range(3):
                    arrived(dc, zv, 1 - core, t)

    for t in range(3):
        local(t).wait()


def gather_rows(key_rows, value_rows, segments):
    grp_n, seq_n = lax.axis_size("grp"), lax.axis_size("seq")
    tok, width = key_rows.shape
    hbm = pl.BlockSpec(memory_space=pl.ANY)
    slots = 3 * seq_n
    return pl.pallas_call(
        functools.partial(spread, grp_n),
        out_shape=[
            jax.ShapeDtypeStruct((slots, tok, width), jnp.bfloat16),
            jax.ShapeDtypeStruct((slots, tok, width), jnp.bfloat16),
            jax.ShapeDtypeStruct((slots, 1, tok), jnp.int32),
        ],
        in_specs=[hbm] * 3,
        out_specs=[hbm] * 3,
        scratch_shapes=[
            pltpu.SemaphoreType.DMA((8, seq_n // 2, 3)),
            pltpu.SemaphoreType.DMA((slots, 3)),
            pltpu.SemaphoreType.DMA((3,)),
        ],
        compiler_params=pltpu.CompilerParams(collective_id=0, has_side_effects=True),
    )(key_rows, value_rows, segments[None, :])


def on_device(queries, key_rows, value_rows, segments):
    tok = queries.shape[0]
    grp_n, seq_n = lax.axis_size("grp"), lax.axis_size("seq")
    device = lax.axis_index(AXES)
    offset = device * tok
    if 2 * seq_n * tok == WINDOW and grp_n % 2 == 0 and seq_n % 2 == 0:
        k_all, v_all, seg_all = gather_rows(key_rows, value_rows, segments)
        base = (lax.axis_index("grp") - 2) * seq_n
    else:
        k_all = lax.all_gather(key_rows, AXES)
        v_all = lax.all_gather(value_rows, AXES)
        seg_all = lax.all_gather(segments, AXES)
        base = 0
    seg_all = seg_all.reshape(-1)
    key_pos = base * tok + jnp.arange(seg_all.shape[0], dtype=jnp.int32)
    begin = jnp.maximum(offset - WINDOW, 0)
    before = (key_pos >= begin) & (key_pos < offset) & (seg_all < segments[0])
    carried = begin + jnp.sum(before.astype(jnp.int32))
    inner = jnp.sum((segments[:, None] < segments[None, :]).astype(jnp.int32), axis=0)
    starts = jnp.where(segments == segments[0], carried, offset + inner)
    positions = offset + jnp.arange(tok, dtype=jnp.int32)
    lower = jnp.maximum(starts, positions - WINDOW + 1)
    first = jnp.min(lower) // tok
    clean = (jnp.max(lower) + tok - 1) // tok
    info = jnp.stack([device, first, clean, device - base]).astype(jnp.int32)
    reach = (WINDOW - 1 + tok - 1) // tok + 1
    return attention(info, lower, queries, k_all, v_all, reach)


def attention(info, lower, queries, k_all, v_all, reach):
    tok = queries.shape[0]
    width = k_all.shape[2]

    def kv_index(j, info):
        return (jnp.maximum(info[3] - j, info[3] - info[0] + info[1]), 0, 0)

    const = lambda j, info: (0, 0)
    return pl.pallas_call(
        flash,
        grid_spec=pltpu.PrefetchScalarGridSpec(
            num_scalar_prefetch=1,
            grid=(reach,),
            in_specs=[
                pl.BlockSpec((1, tok), const),
                pl.BlockSpec(queries.shape, const),
                pl.BlockSpec((None, tok, width), kv_index),
                pl.BlockSpec((None, tok, width), kv_index),
            ],
            out_specs=[
                pl.BlockSpec(queries.shape, const),
                pl.BlockSpec((Q_HEADS, tok), const),
            ],
            scratch_shapes=[
                pltpu.VMEM((Q_HEADS, HEAD_DIM, tok), jnp.bfloat16),
                pltpu.VMEM((Q_HEADS, 1, tok), jnp.float32),
                pltpu.VMEM((Q_HEADS, 1, tok), jnp.float32),
                pltpu.VMEM((Q_HEADS, HEAD_DIM, tok), jnp.float32),
                pltpu.VMEM((tok, tok), jnp.float32),
            ],
        ),
        out_shape=[
            jax.ShapeDtypeStruct(queries.shape, jnp.bfloat16),
            jax.ShapeDtypeStruct((Q_HEADS, tok), jnp.float32),
        ],
        compiler_params=pltpu.CompilerParams(dimension_semantics=("arbitrary",)),
    )(info, lower[None, :], queries, k_all, v_all)


def solution(mesh):
    in_specs = (P(AXES, None), P(AXES, None), P(AXES, None), P(AXES))
    out_specs = (P(AXES, None), P(None, AXES))
    return jax.shard_map(
        on_device, mesh=mesh, in_specs=in_specs, out_specs=out_specs, check_vma=False
    )
```
